256 devices in a mesh: grp: 4 (over z_hi), dev: 64 (over y, x, z_lo, core).
Axes of the slice: x: 4, y: 4, z: 8 (z_hi: 4, z_lo: 2; z = z_hi * 2 + z_lo), core: 2. Of those that a mesh axis runs over, the one named last changes fastest.
Arguments:
- amounts: float32 [64, 4194304], P('dev', 'grp'), may hold values from -0.06 to 0.06, as said below
Outputs:
- offsets: float32 [64, 4194304], P(None, ('grp', 'dev'))
The draws below stay inside these ranges and needn't reach their ends.
Inputs may be any that keep to these rules, and one draw needn't show every extreme that they name: `amounts`: each entry lies within 0.06 of zero.
All inputs are finite; a program needn't handle non-finite values.
Results may differ from the reference program's by a relative error of at most 0.00095.
Values sent between devices are 32-bit elements; how exact they have to be, the bound alone decides.
A program may use at most 64 MiB of HBM per device.

```python
import jax
import jax.numpy as jnp

COLS = 64
ROW_DEV = 16384
ROWS = 4194304


def draw_amounts(key, part):
    subkeys = jax.random.split(jax.random.fold_in(key, 17), 3)
    regions = ROWS // (ROW_DEV // 4)
    noise = jax.random.uniform(subkeys[0], (COLS, ROWS + 1), jnp.float32, -1.0, 1.0)
    reach = 1.0
    drift = jax.random.uniform(subkeys[2], (COLS, 1), jnp.float32, 0.0, 2.0)
    factor = jnp.exp(jax.random.uniform(subkeys[1], (COLS, regions), jnp.float32, -reach, reach))
    factor = jnp.repeat(factor, ROW_DEV // 4, axis=1, total_repeat_length=ROWS)
    rough = 0.01 * (noise[:, 1:] - noise[:, :-1])
    values = factor * (rough + drift / ROWS)
    return values.astype(jnp.float32)


def setup_inputs(seed: int = 0) -> dict:
    arg_keys = jax.random.split(jax.random.key(seed), 2)
    amounts = draw_amounts(jax.random.fold_in(arg_keys[1], 71), 0)
    return {"amounts": amounts}


def exclusive_rows(values, block_len):
    chans, length = values.shape
    blocks = values.reshape(chans, length // block_len, block_len)
    within = jnp.cumsum(blocks, axis=2) - blocks
    sums = jnp.sum(blocks, axis=2)
    starts = jnp.cumsum(sums, axis=1) - sums
    return (within + starts[:, :, None]).reshape(chans, length)


def reference(amounts):
    return exclusive_rows(amounts, 512)
```

```python
import jax
import jax.numpy as jnp
from jax import lax
from jax.experimental import pallas as pl
from jax.experimental.pallas import tpu as pltpu
from jax.sharding import PartitionSpec as P

MESH = pl.DeviceIdType.MESH
LANES = 128
ROWS = 128
N = 64
GROUPS = 4
SPLIT = 2
FIRST = 16


def send_order():
    order = []
    for k in range(N // 2):
        j = (13 * k) % (N // 2)
        for s in range(2):
            order.append(((j // 8 + 2 * s) % 4, ((j // 2) % 4 + 2 * s) % 4, s, j % 2))
    return order[1:]


def split3(v):
    hi = v.astype(jnp.bfloat16)
    rest = v - hi.astype(jnp.float32)
    mid = rest.astype(jnp.bfloat16)
    lo = (rest - mid.astype(jnp.float32)).astype(jnp.bfloat16)
    return hi, mid, lo


def dot(a, b):
    return jnp.dot(a, b, preferred_element_type=jnp.float32)


def gather_kernel(
    x_hbm, buf, xv, lane_w, row_w, part, st, srecv, tot, trecv,
    load_sem, send_sem, recv_sem, small_send, small_recv, tot_send, tot_recv,
):
    me = lax.axis_index("dev")
    grp = lax.axis_index("grp")
    y, x, z, c = me // 16, (me // 4) % 4, (me // 2) % 2, me % 2

    def remote(src, dst, ssem, rsem, dev):
        return pltpu.make_async_remote_copy(
            src_ref=src, dst_ref=dst, send_sem=ssem, recv_sem=rsem,
            device_id={"dev": dev}, device_id_type=MESH,
        )

    load = pltpu.make_async_copy(x_hbm, xv, load_sem)
    load.start()
    barrier = pltpu.get_barrier_semaphore()

    def greet(i, _):
        pl.semaphore_signal(barrier, inc=1, device_id={"dev": (me + i) % N}, device_id_type=MESH)
        return 0

    lax.fori_loop(1, N, greet, 0)
    for i in range(1, GROUPS):
        pl.semaphore_signal(
            barrier, inc=1, device_id={"grp": (grp + i) % GROUPS}, device_id_type=MESH
        )

    r = lax.broadcasted_iota(jnp.int32, (2 * LANES, 2 * LANES), 0) % LANES
    q = lax.broadcasted_iota(jnp.int32, (2 * LANES, 2 * LANES), 1)
    lane_w[...] = ((r < q) | (q >= LANES)).astype(jnp.float32).astype(jnp.bfloat16)
    r = lax.broadcasted_iota(jnp.int32, (ROWS, 2 * ROWS), 0)
    q = lax.broadcasted_iota(jnp.int32, (ROWS, 2 * ROWS), 1) % ROWS
    row_w[...] = (q < r).astype(jnp.float32).astype(jnp.bfloat16)

    pl.semaphore_wait(barrier, N - 1 + GROUPS - 1)

    def send(o):
        t = ((y + o[0]) % 4) * 16 + ((x + o[1]) % 4) * 4 + ((z + o[2]) % 2) * 2 + (c + o[3]) % 2
        h = ROWS // SPLIT
        for i in range(SPLIT):
            remote(
                x_hbm.at[t, pl.ds(i * h, h)], buf.at[me, pl.ds(i * h, h)],
                send_sem, recv_sem.at[me], t,
            ).start()

    order = send_order()
    for o in order[:FIRST]:
        send(o)

    load.wait()

    def range_sum(t, _):
        part[t] = jnp.sum(xv[t].reshape(ROWS // 8, 8, LANES), axis=0)
        return 0

    lax.fori_loop(0, N, range_sum, 0)
    sums = jnp.sum(jnp.sum(part[...], axis=1), axis=1, keepdims=True)
    sums = jnp.broadcast_to(sums, (N, LANES))
    tot[...] = jnp.broadcast_to(jnp.sum(sums, axis=0, keepdims=True), (8, LANES))
    low = row_w[0:N, 0:N]
    a, b, d = split3(sums)
    pre = dot(low, a) + dot(low, b) + dot(low, d)
    trecv[grp] = jnp.zeros((8, LANES), jnp.float32)
    copies = []
    for i in range(1, GROUPS):
        copy = pltpu.make_async_remote_copy(
            src_ref=tot, dst_ref=trecv.at[grp], send_sem=tot_send, recv_sem=tot_recv,
            device_id={"grp": (grp + i) % GROUPS}, device_id_type=MESH,
        )
        copy.start()
    pltpu.make_async_copy(trecv.at[pl.ds(0, 3)], trecv.at[pl.ds(0, 3)], tot_send).wait()
    pltpu.make_async_copy(trecv.at[pl.ds(0, 3)], trecv.at[pl.ds(0, 3)], tot_recv).wait()
    base = jnp.zeros((8, LANES), jnp.float32)
    for i in range(GROUPS - 1):
        base = base + jnp.where(i < grp, trecv[i], 0.0)
    st[...] = pre + base[0:1]

    for o in order:
        t = ((y + o[0]) % 4) * 16 + ((x + o[1]) % 4) * 4 + ((z + o[2]) % 2) * 2 + (c + o[3]) % 2
        remote(st.at[pl.ds(t, 1)], srecv.at[pl.ds(me, 1)], small_send, small_recv, t).start()
    for o in order[FIRST:]:
        send(o)

    def scanned(v, start):
        hi, mid, lo = split3(v)
        both = dot(jnp.concatenate([hi, mid], axis=1), lane_w[...]) + dot(lo, lane_w[0:LANES])
        a, b, d = split3(both[:, LANES:])
        rows = dot(row_w[...], jnp.concatenate([a, b], axis=0)) + dot(row_w[:, 0:ROWS], d)
        return both[:, :LANES] + (rows + start)

    buf[me] = scanned(xv[me], st[pl.ds(me, 1)])
    pltpu.make_async_copy(st.at[pl.ds(0, N - 1)], srecv.at[pl.ds(0, N - 1)], small_recv).wait()

    def receive(i, _):
        k, s = i // 2, i % 2
        j = (13 * k) % (N // 2)
        src = (
            ((y + 8 - j // 8 - 2 * s) % 4) * 16 + ((x + 8 - (j // 2) % 4 - 2 * s) % 4) * 4
            + ((z + s) % 2) * 2 + (c + j) % 2
        )
        pltpu.make_async_copy(buf.at[src], buf.at[src], recv_sem.at[src]).wait()
        buf[src] = scanned(buf[src], srecv[pl.ds(src, 1)])
        return 0

    lax.fori_loop(1, N, receive, 0)
    pltpu.make_async_copy(st.at[pl.ds(0, N - 1)], srecv.at[pl.ds(0, N - 1)], small_send).wait()
    pltpu.make_async_copy(buf.at[pl.ds(0, N - 1)], buf.at[pl.ds(0, N - 1)], send_sem).wait()


def place_kernel(buf, out, sem):
    for t in range(N):
        pltpu.make_async_copy(buf.at[t], out.at[t // 8, :, t % 8], sem).start()
    pltpu.make_async_copy(buf, buf, sem).wait()


def local(amounts):
    slabs = amounts.reshape(N, ROWS, LANES)
    f32, bf16, dma = jnp.float32, jnp.bfloat16, pltpu.SemaphoreType.DMA
    buf = pl.pallas_call(
        gather_kernel,
        out_shape=pltpu.VMEM((N, ROWS, LANES), f32),
        in_specs=[pl.BlockSpec(memory_space=pltpu.HBM)],
        out_specs=pl.BlockSpec(memory_space=pltpu.VMEM),
        scratch_shapes=[
            pltpu.VMEM((N, ROWS, LANES), f32),
            pltpu.VMEM((2 * LANES, 2 * LANES), bf16),
            pltpu.VMEM((ROWS, 2 * ROWS), bf16),
            pltpu.VMEM((N, 8, LANES), f32),
            pltpu.VMEM((N, LANES), f32),
            pltpu.VMEM((N, LANES), f32),
            pltpu.VMEM((8, LANES), f32),
            pltpu.VMEM((GROUPS, 8, LANES), f32),
            dma, dma, dma((N,)), dma, dma, dma, dma,
        ],
        compiler_params=pltpu.CompilerParams(
            collective_id=0, has_side_effects=True, vmem_limit_bytes=56 * 2**20
        ),
    )(slabs)
    out = pl.pallas_call(
        place_kernel,
        out_shape=jax.ShapeDtypeStruct((8, ROWS, 8, LANES), f32),
        in_specs=[pl.BlockSpec(memory_space=pltpu.VMEM)],
        out_specs=pl.BlockSpec(memory_space=pltpu.HBM),
        scratch_shapes=[dma],
        compiler_params=pltpu.CompilerParams(vmem_limit_bytes=8 * 2**20),
    )(pltpu.with_memory_space_constraint(buf, pltpu.VMEM))
    return out.transpose(0, 2, 1, 3).reshape(N, ROWS * LANES)


def solution(mesh):
    return jax.shard_map(
        local,
        mesh=mesh,
        in_specs=(P("dev", "grp"),),
        out_specs=P(None, ("grp", "dev")),
        check_vma=False,
    )
```

```python
import jax
import jax.numpy as jnp
from jax import lax
from jax.experimental import pallas as pl
from jax.experimental.pallas import tpu as pltpu
from jax.sharding import PartitionSpec as P

MESH = pl.DeviceIdType.MESH
LANES = 128
ROWS = 128
N = 64
GROUPS = 4
HALF = ROWS // 2
PLANE = [(0, w // 4, w // 2 % 2, w % 2) for w in range(1, 16)]
LINE = [(i, 0, 0, k) for k in range(2) for i in range(1, 4)]
NEAR = PLANE + LINE
STEP = 4


def order():
    first = [(0, 0, 0, 0), (1, 0, 0, 0), (2, 0, 0, 0), (3, 0, 0, 0)]
    first += [(0, 0, 1, 0), (0, 1, 0, 0), (0, 3, 0, 0), (0, 2, 0, 0)]
    first += [(0, 0, 0, 1), (1, 0, 0, 1), (2, 0, 0, 1), (3, 0, 0, 1)]
    near = [o for o in PLANE if o not in first]
    far = [[(1 + k, w // 4, w // 2 % 2, w % 2) for w in range(2, 16)] for k in range(3)]
    rest = []
    for i in range(14):
        rest += [far[k][(5 * i + 4 * k) % 14] for k in range(3)]
        if i * 10 // 14 != (i + 1) * 10 // 14:
            rest.append(near[(3 * len(rest) // 5) % len(near)])
            near.remove(rest[-1])
    return first + rest


ORDER = order()
NOW = 12
TOTAL_AT = 6


def pick(i, values):
    r = values[0]
    for k, v in enumerate(values[1:], 1):
        r = jnp.where(i == k, v, r)
    return r


def split3(v):
    hi = v.astype(jnp.bfloat16)
    rest = v - hi.astype(jnp.float32)
    mid = rest.astype(jnp.bfloat16)
    lo = (rest - mid.astype(jnp.float32)).astype(jnp.bfloat16)
    return hi, mid, lo


def dot(a, b):
    return jnp.dot(a, b, preferred_element_type=jnp.float32)


def gather_kernel(
    x_hbm, buf, xv, lane_w, row_w, part, starts, tot, trecv,
    load_sem, send_sem, recv_sem, tot_send, tot_recv, row_sem, ready_sem,
):
    me = lax.axis_index("dev")
    grp = lax.axis_index("grp")
    y, x, z, c = me // 16, (me // 4) % 4, (me // 2) % 2, me % 2

    def remote(src, dst, ssem, rsem, dev):
        return pltpu.make_async_remote_copy(
            src_ref=src, dst_ref=dst, send_sem=ssem, recv_sem=rsem,
            device_id={"dev": dev}, device_id_type=MESH,
        )

    loads = []
    for i in range(4):
        ts = pl.ds(((y + i) % 4) * 16, 16)
        loads.append(pltpu.make_async_copy(x_hbm.at[ts], xv.at[ts, pl.ds(0, ROWS)], load_sem.at[i]))
        loads[-1].start()
    barrier = pltpu.get_barrier_semaphore()

    def device(o, sign=1):
        return (
            ((y + sign * o[0] + 4) % 4) * 16
            + ((x + sign * o[1] + 4) % 4) * 4
            + ((z + o[2]) % 2) * 2
            + (c + o[3]) % 2
        )

    for o in NEAR:
        pl.semaphore_signal(barrier, inc=1, device_id={"dev": device(o)}, device_id_type=MESH)

    def greet(g, _):
        pl.semaphore_signal(barrier, inc=1, device_id={"grp": g}, device_id_type=MESH)
        return 0

    lax.fori_loop(grp + 1, GROUPS, greet, 0)

    r = lax.broadcasted_iota(jnp.int32, (2 * LANES, 2 * LANES), 0) % LANES
    q = lax.broadcasted_iota(jnp.int32, (2 * LANES, 2 * LANES), 1)
    lane_w[...] = ((r < q) | (q >= LANES)).astype(jnp.float32).astype(jnp.bfloat16)
    r = lax.broadcasted_iota(jnp.int32, (ROWS, 2 * ROWS), 0)
    q = lax.broadcasted_iota(jnp.int32, (ROWS, 2 * ROWS), 1) % ROWS
    row_w[...] = (q < r).astype(jnp.float32).astype(jnp.bfloat16)

    def scan(ts):
        v = jnp.concatenate([xv[t, 0:ROWS] for t in ts], axis=0)
        hi, mid, lo = split3(v)
        both = dot(jnp.concatenate([hi, mid], axis=1), lane_w[...]) + dot(lo, lane_w[0:LANES])
        out = []
        for k in range(len(ts)):
            rows = slice(k * ROWS, (k + 1) * ROWS)
            a, b, d = split3(both[rows, LANES:])
            before = dot(row_w[...], jnp.concatenate([a, b], axis=0)) + dot(row_w[:, 0:ROWS], d)
            out.append(both[rows, :LANES] + before)
        for t, v in zip(ts, out):
            xv[t, 0:ROWS] = v

    def send(t, first, rows):
        rows = pl.ds(first, rows)
        remote(xv.at[t, rows], buf.at[me, rows], send_sem, recv_sem.at[me], t).start()

    for load in loads:
        load.wait()

    def range_sum(t, _):
        part[t] = jnp.sum(xv[t, 0:ROWS].reshape(ROWS // 8, 8, LANES), axis=0)
        return 0

    lax.fori_loop(0, N, range_sum, 0)
    scan([device(o) for o in ORDER[0:STEP]])
    sums = jnp.sum(jnp.sum(part[...], axis=1), axis=1, keepdims=True)
    sums = jnp.broadcast_to(sums, (N, LANES))
    tot[...] = jnp.broadcast_to(jnp.sum(sums, axis=0, keepdims=True), (8, LANES))
    low = row_w[0:N, 0:N]
    a, b, d = split3(sums)
    starts[...] = dot(low, a) + dot(low, b) + dot(low, d)

    pl.semaphore_wait(barrier, len(NEAR) + grp)
    def ready(g, _):
        pl.semaphore_signal(ready_sem, inc=1, device_id={"grp": g}, device_id_type=MESH)
        return 0

    lax.fori_loop(0, grp, ready, 0)
    for i in range(1, 4):
        pl.semaphore_signal(
            row_sem, inc=1, device_id={"dev": device((i, 0, 0, 0))}, device_id_type=MESH
        )
    for o in ORDER[1:STEP]:
        send(device(o), 0, HALF)
    for i in range(STEP, NOW, STEP):
        ts = [device(o) for o in ORDER[i : i + STEP]]
        scan(ts)
        for t in ts:
            send(t, 0, HALF)

    pl.semaphore_wait(row_sem, 3)

    table = [[o[k] for o in ORDER] for k in range(4)]

    def offset(i, m):
        return [pick(i, values[m::STEP]) for values in table]

    def targets(i):
        return [device(offset(i, m)) for m in range(STEP)]

    def scan_and_send(i, _):
        ts = targets(i)
        scan(ts)
        for t in ts:
            send(t, 0, HALF)
        return 0

    lax.fori_loop(NOW // STEP, TOTAL_AT, scan_and_send, 0)

    def send_total(g, _):
        pltpu.make_async_remote_copy(
            src_ref=tot, dst_ref=trecv.at[grp], send_sem=tot_send.at[g], recv_sem=tot_recv.at[grp],
            device_id={"grp": g}, device_id_type=MESH,
        ).start()
        return 0

    @pl.when(grp < GROUPS - 1)
    def _():
        pl.semaphore_wait(ready_sem, GROUPS - 1 - grp)

    lax.fori_loop(grp + 1, GROUPS, send_total, 0)

    lax.fori_loop(TOTAL_AT, N // STEP, scan_and_send, 0)

    def add_total(g, base):
        pltpu.make_async_copy(tot, tot, tot_recv.at[g]).wait()
        return base + trecv[g]

    base = lax.fori_loop(0, grp, add_total, jnp.zeros((8, LANES), jnp.float32))

    def put_start(t, _):
        start = starts[pl.ds(t, 1)] + base[0:1]
        xv[t, HALF:ROWS] += start
        xv[t, ROWS:] = jnp.broadcast_to(start, (8, LANES))
        return 0

    lax.fori_loop(0, N, put_start, 0)
    for o in ORDER[1:]:
        send(device(o), HALF, HALF + 1)
    buf[me, 0:HALF] = xv[me, 0:HALF] + xv[me, ROWS : ROWS + 1]
    buf[me, HALF:ROWS] = xv[me, HALF:ROWS]

    def receive(src):
        slab = buf.at[src, pl.ds(0, ROWS + 1)]
        pltpu.make_async_copy(slab, slab, recv_sem.at[src]).wait()
        buf[src, 0:HALF] += buf[src, ROWS : ROWS + 1]

    for o in ORDER[1:]:
        receive(device(o, -1))

    def total_sent(g, _):
        pltpu.make_async_copy(tot, tot, tot_send.at[g]).wait()
        return 0

    lax.fori_loop(grp + 1, GROUPS, total_sent, 0)
    sent = buf.at[pl.ds(0, N - 1), pl.ds(0, ROWS + 1)]
    pltpu.make_async_copy(sent, sent, send_sem).wait()


def place_kernel(buf, out, sem):
    for t in range(N):
        pltpu.make_async_copy(buf.at[t, pl.ds(0, ROWS)], out.at[t // 8, :, t % 8], sem).start()
    pltpu.make_async_copy(out, out, sem).wait()


def local(amounts):
    slabs = amounts.reshape(N, ROWS, LANES)
    f32, bf16, dma = jnp.float32, jnp.bfloat16, pltpu.SemaphoreType.DMA
    buf = pl.pallas_call(
        gather_kernel,
        out_shape=pltpu.VMEM((N, ROWS + 8, LANES), f32),
        in_specs=[pl.BlockSpec(memory_space=pltpu.HBM)],
        out_specs=pl.BlockSpec(memory_space=pltpu.VMEM),
        scratch_shapes=[
            pltpu.VMEM((N, ROWS + 8, LANES), f32),
            pltpu.VMEM((2 * LANES, 2 * LANES), bf16),
            pltpu.VMEM((ROWS, 2 * ROWS), bf16),
            pltpu.VMEM((N, 8, LANES), f32),
            pltpu.VMEM((N, LANES), f32),
            pltpu.VMEM((8, LANES), f32),
            pltpu.VMEM((GROUPS, 8, LANES), f32),
            dma((4,)), dma, dma((N,)), dma((GROUPS,)), dma((GROUPS,)),
            pltpu.SemaphoreType.REGULAR, pltpu.SemaphoreType.REGULAR,
        ],
        compiler_params=pltpu.CompilerParams(
            collective_id=0, has_side_effects=True, vmem_limit_bytes=56 * 2**20
        ),
    )(slabs)
    out = pl.pallas_call(
        place_kernel,
        out_shape=jax.ShapeDtypeStruct((8, ROWS, 8, LANES), f32),
        in_specs=[pl.BlockSpec(memory_space=pltpu.VMEM)],
        out_specs=pl.BlockSpec(memory_space=pltpu.HBM),
        scratch_shapes=[dma],
        compiler_params=pltpu.CompilerParams(vmem_limit_bytes=8 * 2**20),
    )(pltpu.with_memory_space_constraint(buf, pltpu.VMEM))
    return out.transpose(0, 2, 1, 3).reshape(N, ROWS * LANES)


def solution(mesh):
    return jax.shard_map(
        local,
        mesh=mesh,
        in_specs=(P("dev", "grp"),),
        out_specs=P(None, ("grp", "dev")),
        check_vma=False,
    )
```

```python
import jax
import jax.numpy as jnp
from jax import lax
from jax.experimental import pallas as pl
from jax.experimental.pallas import tpu as pltpu
from jax.sharding import PartitionSpec as P

MESH = pl.DeviceIdType.MESH
LANES = 128
ROWS = 128
N = 64
GROUPS = 4
HALF = ROWS // 2
PLANE = [(0, w // 4, w // 2 % 2, w % 2) for w in range(1, 16)]
LINE = [(i, 0, 0, k) for k in range(2) for i in range(1, 4)]
NEAR = PLANE + LINE
STEP = 4


def order():
    first = [(0, 0, 0, 0), (0, 0, 1, 0), (0, 1, 0, 0), (0, 3, 0, 0)]
    first += [(1, 0, 0, 0), (3, 0, 0, 0), (0, 0, 1, 1), (0, 1, 0, 1)]
    first += [(0, 3, 0, 1), (1, 0, 0, 1), (3, 0, 0, 1), (0, 0, 0, 1)]
    near = [o for o in NEAR if o not in first]
    far = [[(1 + k, w // 4, w // 2 % 2, w % 2) for w in range(2, 16)] for k in range(3)]
    rest = []
    for i in range(14):
        rest += [far[k][(5 * i + 4 * k) % 14] for k in range(3)]
        if i * 10 // 14 != (i + 1) * 10 // 14:
            rest.append(near[(3 * len(rest) // 5) % len(near)])
            near.remove(rest[-1])
    return first + rest


ORDER = order()
NOW = 12
SOON = 36


def pick(i, values):
    r = values[0]
    for k, v in enumerate(values[1:], 1):
        r = jnp.where(i == k, v, r)
    return r


def split3(v):
    hi = v.astype(jnp.bfloat16)
    rest = v - hi.astype(jnp.float32)
    mid = rest.astype(jnp.bfloat16)
    lo = (rest - mid.astype(jnp.float32)).astype(jnp.bfloat16)
    return hi, mid, lo


def dot(a, b):
    return jnp.dot(a, b, preferred_element_type=jnp.float32)


def gather_kernel(
    x_hbm, buf, xr, xv, lane_w, row_w, part, starts, halves, tot, trecv,
    load_sem, send_sem, first_sem, second_sem, tot_send, tot_recv, row_sem, ready_sem,
):
    me = lax.axis_index("dev")
    grp = lax.axis_index("grp")
    y, x, z, c = me // 16, (me // 4) % 4, (me // 2) % 2, me % 2

    def remote(src, dst, ssem, rsem, dev):
        return pltpu.make_async_remote_copy(
            src_ref=src, dst_ref=dst, send_sem=ssem, recv_sem=rsem,
            device_id={"dev": dev}, device_id_type=MESH,
        )

    loads = []
    for i in range(4):
        ts = pl.ds(((y + i) % 4) * 16, 16)
        loads.append(pltpu.make_async_copy(x_hbm.at[ts], xr.at[ts], load_sem.at[i]))
        loads[-1].start()
    barrier = pltpu.get_barrier_semaphore()

    def device(o, sign=1):
        return (
            ((y + sign * o[0] + 4) % 4) * 16
            + ((x + sign * o[1] + 4) % 4) * 4
            + ((z + o[2]) % 2) * 2
            + (c + o[3]) % 2
        )

    for o in NEAR:
        pl.semaphore_signal(barrier, inc=1, device_id={"dev": device(o)}, device_id_type=MESH)

    def greet(g, _):
        pl.semaphore_signal(barrier, inc=1, device_id={"grp": g}, device_id_type=MESH)
        return 0

    lax.fori_loop(grp + 1, GROUPS, greet, 0)

    pl.semaphore_wait(barrier, len(NEAR) + grp)
    for i in range(1, 4):
        pl.semaphore_signal(
            row_sem, inc=1, device_id={"dev": device((i, 0, 0, 0))}, device_id_type=MESH
        )

    def send_first(order):
        half = pl.ds(0, HALF)
        for o in order:
            t = device(o)
            remote(x_hbm.at[t, half], buf.at[me, half], send_sem, first_sem.at[me], t).start()

    send_first(ORDER[1:NOW])

    def ready(g, _):
        pl.semaphore_signal(ready_sem, inc=1, device_id={"grp": g}, device_id_type=MESH)
        return 0

    lax.fori_loop(0, grp, ready, 0)

    r = lax.broadcasted_iota(jnp.int32, (2 * LANES, 2 * LANES), 0) % LANES
    q = lax.broadcasted_iota(jnp.int32, (2 * LANES, 2 * LANES), 1)
    lane_w[...] = ((r < q) | (q >= LANES)).astype(jnp.float32).astype(jnp.bfloat16)
    r = lax.broadcasted_iota(jnp.int32, (ROWS, 2 * ROWS), 0)
    q = lax.broadcasted_iota(jnp.int32, (ROWS, 2 * ROWS), 1) % ROWS
    row_w[...] = (q < r).astype(jnp.float32).astype(jnp.bfloat16)

    def lane_scan(v):
        hi, mid, lo = split3(v)
        return dot(jnp.concatenate([hi, mid], axis=1), lane_w[...]) + dot(lo, lane_w[0:LANES])

    def scan(ts):
        both = lane_scan(jnp.concatenate([xr[t] for t in ts], axis=0))
        out = []
        for k in range(len(ts)):
            rows = slice(k * ROWS, (k + 1) * ROWS)
            a, b, d = split3(both[rows, LANES:])
            before = dot(row_w[...], jnp.concatenate([a, b], axis=0)) + dot(row_w[:, 0:ROWS], d)
            out.append(both[rows, :LANES] + before)
        for t, v in zip(ts, out):
            xv[t] = v

    pl.semaphore_wait(row_sem, 3)
    send_first(ORDER[NOW:SOON])
    for load in loads:
        load.wait()

    def range_sum(t, _):
        part[t] = jnp.sum(xr[t].reshape(ROWS // 8, 8, LANES), axis=0)
        return 0

    lax.fori_loop(0, N, range_sum, 0)
    sums = jnp.sum(jnp.sum(part[...], axis=1), axis=1, keepdims=True)
    sums = jnp.broadcast_to(sums, (N, LANES))
    tot[...] = jnp.broadcast_to(jnp.sum(sums, axis=0, keepdims=True), (8, LANES))
    low = row_w[0:N, 0:N]
    a, b, d = split3(sums)
    starts[...] = dot(low, a) + dot(low, b) + dot(low, d)

    @pl.when(grp < GROUPS - 1)
    def _():
        pl.semaphore_wait(ready_sem, GROUPS - 1 - grp)

    def send_total(g, _):
        pltpu.make_async_remote_copy(
            src_ref=tot, dst_ref=trecv.at[grp], send_sem=tot_send.at[g], recv_sem=tot_recv.at[grp],
            device_id={"grp": g}, device_id_type=MESH,
        ).start()
        return 0

    lax.fori_loop(grp + 1, GROUPS, send_total, 0)
    send_first(ORDER[SOON:])

    table = [[o[k] for o in ORDER] for k in range(4)]

    def devices(i, sign=1):
        return [device([pick(i, v[m::STEP]) for v in table], sign) for m in range(STEP)]

    def scan_step(i, _):
        scan(devices(i))
        return 0

    lax.fori_loop(0, N // STEP, scan_step, 0)

    def add_total(g, base):
        pltpu.make_async_copy(tot, tot, tot_recv.at[g]).wait()
        return base + trecv[g]

    base = lax.fori_loop(0, grp, add_total, jnp.zeros((8, LANES), jnp.float32))

    def put_start(t, _):
        xv[t] += starts[pl.ds(t, 1)] + base[0:1]
        return 0

    lax.fori_loop(0, N, put_start, 0)
    for o in ORDER[1:]:
        t, half = device(o), pl.ds(HALF, HALF)
        remote(xv.at[t, half], buf.at[me, half], send_sem, second_sem.at[me], t).start()
    buf[me] = xv[me]

    low_half = row_w[0:HALF, 0:HALF]

    def scan_first(srcs):
        for src in srcs:
            half = buf.at[src, pl.ds(0, HALF)]
            pltpu.make_async_copy(half, half, first_sem.at[src]).wait()
        both = lane_scan(jnp.concatenate([buf[src, 0:HALF] for src in srcs], axis=0))
        out = []
        for k in range(len(srcs)):
            rows = slice(k * HALF, (k + 1) * HALF)
            sums = both[rows, LANES:]
            a, b, d = split3(sums)
            before = dot(low_half, a) + dot(low_half, b) + dot(low_half, d)
            out.append((both[rows, :LANES] + before, (before + sums)[HALF - 1 :]))
        for src, (v, total) in zip(srcs, out):
            buf[src, 0:HALF] = v
            halves[pl.ds(src, 1)] = total

    scan_first([device(o, -1) for o in ORDER[1:STEP]])

    def first_step(i, _):
        scan_first(devices(i, -1))
        return 0

    lax.fori_loop(1, N // STEP, first_step, 0)

    for o in ORDER[1:]:
        src = device(o, -1)
        half = buf.at[src, pl.ds(HALF, HALF)]
        pltpu.make_async_copy(half, half, second_sem.at[src]).wait()
        start = jnp.broadcast_to(buf[src, HALF : HALF + 1, 0:1], (1, LANES)) - halves[pl.ds(src, 1)]
        buf[src, 0:HALF] += start

    def total_sent(g, _):
        pltpu.make_async_copy(tot, tot, tot_send.at[g]).wait()
        return 0

    lax.fori_loop(grp + 1, GROUPS, total_sent, 0)
    sent = buf.at[pl.ds(0, N - 1)]
    pltpu.make_async_copy(sent, sent, send_sem).wait()


def place_kernel(buf, out, sem):
    for t in range(N):
        pltpu.make_async_copy(buf.at[t], out.at[t // 8, :, t % 8], sem).start()
    pltpu.make_async_copy(out, out, sem).wait()


def local(amounts):
    slabs = amounts.reshape(N, ROWS, LANES)
    f32, bf16, dma = jnp.float32, jnp.bfloat16, pltpu.SemaphoreType.DMA
    buf = pl.pallas_call(
        gather_kernel,
        out_shape=pltpu.VMEM((N, ROWS, LANES), f32),
        in_specs=[pl.BlockSpec(memory_space=pltpu.HBM)],
        out_specs=pl.BlockSpec(memory_space=pltpu.VMEM),
        scratch_shapes=[
            pltpu.VMEM((N, ROWS, LANES), f32),
            pltpu.VMEM((N, ROWS, LANES), f32),
            pltpu.VMEM((2 * LANES, 2 * LANES), bf16),
            pltpu.VMEM((ROWS, 2 * ROWS), bf16),
            pltpu.VMEM((N, 8, LANES), f32),
            pltpu.VMEM((N, LANES), f32),
            pltpu.VMEM((N, LANES), f32),
            pltpu.VMEM((8, LANES), f32),
            pltpu.VMEM((GROUPS, 8, LANES), f32),
            dma((4,)), dma, dma((N,)), dma((N,)), dma((GROUPS,)), dma((GROUPS,)),
            pltpu.SemaphoreType.REGULAR, pltpu.SemaphoreType.REGULAR,
        ],
        compiler_params=pltpu.CompilerParams(
            collective_id=0, has_side_effects=True, vmem_limit_bytes=56 * 2**20
        ),
    )(slabs)
    out = pl.pallas_call(
        place_kernel,
        out_shape=jax.ShapeDtypeStruct((8, ROWS, 8, LANES), f32),
        in_specs=[pl.BlockSpec(memory_space=pltpu.VMEM)],
        out_specs=pl.BlockSpec(memory_space=pltpu.HBM),
        scratch_shapes=[dma],
        compiler_params=pltpu.CompilerParams(vmem_limit_bytes=8 * 2**20),
    )(pltpu.with_memory_space_constraint(buf, pltpu.VMEM))
    return out.transpose(0, 2, 1, 3).reshape(N, ROWS * LANES)


def solution(mesh):
    return jax.shard_map(
        local,
        mesh=mesh,
        in_specs=(P("dev", "grp"),),
        out_specs=P(None, ("grp", "dev")),
        check_vma=False,
    )
```

```python
import jax
import jax.numpy as jnp
from jax import lax
from jax.experimental import pallas as pl
from jax.experimental.pallas import tpu as pltpu
from jax.sharding import PartitionSpec as P

MESH = pl.DeviceIdType.MESH
LANES = 128
ROWS = 128
N = 64
GROUPS = 4
HALF = ROWS // 2
PLANE = [(0, w // 4, w // 2 % 2, w % 2) for w in range(1, 16)]
LINE = [(i, 0, 0, k) for k in range(2) for i in range(1, 4)]
NEAR = PLANE + LINE
STEP = 4


def order():
    first = [(0, 0, 0, 0)]
    for k in range(2):
        first += [(0, 0, 1, k), (0, 1, 0, k), (1, 0, 0, k), (0, 3, 0, k), (3, 0, 0, k)]
    first.append((0, 0, 0, 1))
    near = [(2, 0, 0, 0), (0, 2, 0, 0), (2, 0, 0, 1), (0, 1, 1, 1), (0, 3, 1, 0)]
    near += [(0, 2, 1, 0), (0, 2, 0, 1), (0, 1, 1, 0), (0, 3, 1, 1), (0, 2, 1, 1)]
    far = [[(1 + k, w // 4, w // 2 % 2, w % 2) for w in range(2, 16)] for k in range(3)]
    rest = []
    for i in range(14):
        rest += [far[k][(5 * i + 4 * k + 3) % 14] for k in range(3)]
        if i * 10 // 14 != (i + 1) * 10 // 14:
            rest.append(near.pop((3 * len(rest) // 5) % len(near)))
    return first + rest


ORDER = order()
NOW = 12
SOON = 36


def pick(i, values):
    r = values[0]
    for k, v in enumerate(values[1:], 1):
        r = jnp.where(i == k, v, r)
    return r


def split3(v):
    hi = v.astype(jnp.bfloat16)
    rest = v - hi.astype(jnp.float32)
    mid = rest.astype(jnp.bfloat16)
    lo = (rest - mid.astype(jnp.float32)).astype(jnp.bfloat16)
    return hi, mid, lo


def dot(a, b):
    return jnp.dot(a, b, preferred_element_type=jnp.float32)


def gather_kernel(
    x_hbm, buf, xr, xv, lane_w, row_w, part, starts, halves, tot, trecv,
    load_sem, send_sem, first_sem, second_sem, tot_send, tot_recv, row_sem, ready_sem,
):
    me = lax.axis_index("dev")
    grp = lax.axis_index("grp")
    y, x, z, c = me // 16, (me // 4) % 4, (me // 2) % 2, me % 2

    def remote(src, dst, ssem, rsem, dev):
        return pltpu.make_async_remote_copy(
            src_ref=src, dst_ref=dst, send_sem=ssem, recv_sem=rsem,
            device_id={"dev": dev}, device_id_type=MESH,
        )

    loads = []
    for i in range(4):
        ts = pl.ds(((y + i) % 4) * 16, 16)
        loads.append(pltpu.make_async_copy(x_hbm.at[ts], xr.at[ts], load_sem.at[i]))
        loads[-1].start()
    barrier = pltpu.get_barrier_semaphore()

    def device(o, sign=1):
        return (
            ((y + sign * o[0] + 4) % 4) * 16
            + ((x + sign * o[1] + 4) % 4) * 4
            + ((z + o[2]) % 2) * 2
            + (c + o[3]) % 2
        )

    for o in NEAR:
        pl.semaphore_signal(barrier, inc=1, device_id={"dev": device(o)}, device_id_type=MESH)

    def greet(g, _):
        pl.semaphore_signal(barrier, inc=1, device_id={"grp": g}, device_id_type=MESH)
        return 0

    lax.fori_loop(grp + 1, GROUPS, greet, 0)

    pl.semaphore_wait(barrier, len(NEAR) + grp)
    for i in range(1, 4):
        pl.semaphore_signal(
            row_sem, inc=1, device_id={"dev": device((i, 0, 0, 0))}, device_id_type=MESH
        )

    def send_first(order):
        half = pl.ds(0, HALF)
        for o in order:
            t = device(o)
            remote(x_hbm.at[t, half], buf.at[me, half], send_sem, first_sem.at[me], t).start()

    send_first(ORDER[1:NOW])

    def ready(g, _):
        pl.semaphore_signal(ready_sem, inc=1, device_id={"grp": g}, device_id_type=MESH)
        return 0

    lax.fori_loop(0, grp, ready, 0)

    r = lax.broadcasted_iota(jnp.int32, (2 * LANES, 2 * LANES), 0) % LANES
    q = lax.broadcasted_iota(jnp.int32, (2 * LANES, 2 * LANES), 1)
    lane_w[...] = ((r < q) | (q >= LANES)).astype(jnp.float32).astype(jnp.bfloat16)
    r = lax.broadcasted_iota(jnp.int32, (ROWS, 2 * ROWS), 0)
    q = lax.broadcasted_iota(jnp.int32, (ROWS, 2 * ROWS), 1) % ROWS
    row_w[...] = (q < r).astype(jnp.float32).astype(jnp.bfloat16)

    def lane_scan(v):
        hi, mid, lo = split3(v)
        return dot(jnp.concatenate([hi, mid], axis=1), lane_w[...]) + dot(lo, lane_w[0:LANES])

    def scan(ts):
        both = lane_scan(jnp.concatenate([xr[t] for t in ts], axis=0))
        out = []
        for k in range(len(ts)):
            rows = slice(k * ROWS, (k + 1) * ROWS)
            a, b, d = split3(both[rows, LANES:])
            before = dot(row_w[...], jnp.concatenate([a, b], axis=0)) + dot(row_w[:, 0:ROWS], d)
            out.append(both[rows, :LANES] + before)
        for t, v in zip(ts, out):
            xv[t] = v

    pl.semaphore_wait(row_sem, 3)
    send_first(ORDER[NOW:SOON])
    for load in loads:
        load.wait()

    def range_sum(t, _):
        part[t] = jnp.sum(xr[t].reshape(ROWS // 8, 8, LANES), axis=0)
        return 0

    lax.fori_loop(0, N, range_sum, 0)
    sums = jnp.sum(jnp.sum(part[...], axis=1), axis=1, keepdims=True)
    sums = jnp.broadcast_to(sums, (N, LANES))
    tot[...] = jnp.broadcast_to(jnp.sum(sums, axis=0, keepdims=True), (8, LANES))
    low = row_w[0:N, 0:N]
    a, b, d = split3(sums)
    starts[...] = dot(low, a) + dot(low, b) + dot(low, d)

    @pl.when(grp < GROUPS - 1)
    def _():
        pl.semaphore_wait(ready_sem, GROUPS - 1 - grp)

    def send_total(g, _):
        pltpu.make_async_remote_copy(
            src_ref=tot, dst_ref=trecv.at[grp], send_sem=tot_send.at[g], recv_sem=tot_recv.at[grp],
            device_id={"grp": g}, device_id_type=MESH,
        ).start()
        return 0

    lax.fori_loop(grp + 1, GROUPS, send_total, 0)
    send_first(ORDER[SOON:])

    table = [[o[k] for o in ORDER] for k in range(4)]

    def devices(i, sign=1):
        return [device([pick(i, v[m::STEP]) for v in table], sign) for m in range(STEP)]

    def scan_step(i, _):
        scan(devices(i))
        return 0

    lax.fori_loop(0, N // STEP, scan_step, 0)

    def add_total(g, base):
        pltpu.make_async_copy(tot, tot, tot_recv.at[g]).wait()
        return base + trecv[g]

    base = lax.fori_loop(0, grp, add_total, jnp.zeros((8, LANES), jnp.float32))

    def put_start(t, _):
        xv[t] += starts[pl.ds(t, 1)] + base[0:1]
        return 0

    lax.fori_loop(0, N, put_start, 0)
    for o in ORDER[1:]:
        t, half = device(o), pl.ds(HALF, HALF)
        remote(xv.at[t, half], buf.at[me, half], send_sem, second_sem.at[me], t).start()
    buf[me] = xv[me]

    low_half = row_w[0:HALF, 0:HALF]

    def scan_first(srcs):
        for src in srcs:
            half = buf.at[src, pl.ds(0, HALF)]
            pltpu.make_async_copy(half, half, first_sem.at[src]).wait()
        both = lane_scan(jnp.concatenate([buf[src, 0:HALF] for src in srcs], axis=0))
        out = []
        for k in range(len(srcs)):
            rows = slice(k * HALF, (k + 1) * HALF)
            sums = both[rows, LANES:]
            a, b, d = split3(sums)
            before = dot(low_half, a) + dot(low_half, b) + dot(low_half, d)
            out.append((both[rows, :LANES] + before, (before + sums)[HALF - 1 :]))
        for src, (v, total) in zip(srcs, out):
            buf[src, 0:HALF] = v
            halves[pl.ds(src, 1)] = total

    scan_first([device(o, -1) for o in ORDER[1:STEP]])

    def first_step(i, _):
        scan_first(devices(i, -1))
        return 0

    lax.fori_loop(1, N // STEP, first_step, 0)

    for o in ORDER[1:]:
        src = device(o, -1)
        half = buf.at[src, pl.ds(HALF, HALF)]
        pltpu.make_async_copy(half, half, second_sem.at[src]).wait()
        start = jnp.broadcast_to(buf[src, HALF : HALF + 1, 0:1], (1, LANES)) - halves[pl.ds(src, 1)]
        buf[src, 0:HALF] += start

    def total_sent(g, _):
        pltpu.make_async_copy(tot, tot, tot_send.at[g]).wait()
        return 0

    lax.fori_loop(grp + 1, GROUPS, total_sent, 0)
    sent = buf.at[pl.ds(0, N - 1)]
    pltpu.make_async_copy(sent, sent, send_sem).wait()


def place_kernel(buf, out, sem):
    for t in range(N):
        pltpu.make_async_copy(buf.at[t], out.at[t // 8, :, t % 8], sem).start()
    pltpu.make_async_copy(out, out, sem).wait()


def local(amounts):
    slabs = amounts.reshape(N, ROWS, LANES)
    f32, bf16, dma = jnp.float32, jnp.bfloat16, pltpu.SemaphoreType.DMA
    buf = pl.pallas_call(
        gather_kernel,
        out_shape=pltpu.VMEM((N, ROWS, LANES), f32),
        in_specs=[pl.BlockSpec(memory_space=pltpu.HBM)],
        out_specs=pl.BlockSpec(memory_space=pltpu.VMEM),
        scratch_shapes=[
            pltpu.VMEM((N, ROWS, LANES), f32),
            pltpu.VMEM((N, ROWS, LANES), f32),
            pltpu.VMEM((2 * LANES, 2 * LANES), bf16),
            pltpu.VMEM((ROWS, 2 * ROWS), bf16),
            pltpu.VMEM((N, 8, LANES), f32),
            pltpu.VMEM((N, LANES), f32),
            pltpu.VMEM((N, LANES), f32),
            pltpu.VMEM((8, LANES), f32),
            pltpu.VMEM((GROUPS, 8, LANES), f32),
            dma((4,)), dma, dma((N,)), dma((N,)), dma((GROUPS,)), dma((GROUPS,)),
            pltpu.SemaphoreType.REGULAR, pltpu.SemaphoreType.REGULAR,
        ],
        compiler_params=pltpu.CompilerParams(
            collective_id=0, has_side_effects=True, vmem_limit_bytes=56 * 2**20
        ),
    )(slabs)
    out = pl.pallas_call(
        place_kernel,
        out_shape=jax.ShapeDtypeStruct((8, ROWS, 8, LANES), f32),
        in_specs=[pl.BlockSpec(memory_space=pltpu.VMEM)],
        out_specs=pl.BlockSpec(memory_space=pltpu.HBM),
        scratch_shapes=[dma],
        compiler_params=pltpu.CompilerParams(vmem_limit_bytes=8 * 2**20),
    )(pltpu.with_memory_space_constraint(buf, pltpu.VMEM))
    return out.transpose(0, 2, 1, 3).reshape(N, ROWS * LANES)


def solution(mesh):
    return jax.shard_map(
        local,
        mesh=mesh,
        in_specs=(P("dev", "grp"),),
        out_specs=P(None, ("grp", "dev")),
        check_vma=False,
    )
```

```python
import jax
import jax.numpy as jnp
from jax import lax
from jax.experimental import pallas as pl
from jax.experimental.pallas import tpu as pltpu
from jax.sharding import PartitionSpec as P

MESH = pl.DeviceIdType.MESH
LANES = 128
ROWS = 128
N = 64
GROUPS = 4
HALF = ROWS // 2
PLANE = [(0, w // 4, w // 2 % 2, w % 2) for w in range(1, 16)]
LINE = [(i, 0, 0, k) for k in range(2) for i in range(1, 4)]
NEAR = PLANE[::-1] + LINE
STEP = 4
LAST = 8


def order():
    first = [(0, 0, 0, 0)]
    for k in range(2):
        first += [(0, 0, 1, k), (0, 1, 0, k), (1, 0, 0, k), (0, 3, 0, k), (3, 0, 0, k)]
    first.append((0, 0, 0, 1))
    near = [(2, 0, 0, 0), (0, 2, 0, 0), (2, 0, 0, 1), (0, 1, 1, 1), (0, 3, 1, 0)]
    near += [(0, 2, 1, 0), (0, 2, 0, 1), (0, 1, 1, 0), (0, 3, 1, 1), (0, 2, 1, 1)]
    far = [[(1 + k, w // 4, w // 2 % 2, w % 2) for w in range(2, 16)] for k in range(3)]
    rest = []
    for i in range(14):
        rest += [far[k][(5 * i + 4 * k + 3) % 14] for k in range(3)]
        if i * 10 // 14 != (i + 1) * 10 // 14:
            rest.append(near.pop((3 * len(rest) // 5) % len(near)))
    return first + rest


ORDER = order()
NOW = 12
SOON = 36


def pick(i, values):
    r = values[0]
    for k, v in enumerate(values[1:], 1):
        r = jnp.where(i == k, v, r)
    return r


def split3(v):
    hi = v.astype(jnp.bfloat16)
    rest = v - hi.astype(jnp.float32)
    mid = rest.astype(jnp.bfloat16)
    lo = (rest - mid.astype(jnp.float32)).astype(jnp.bfloat16)
    return hi, mid, lo


def dot(a, b):
    return jnp.dot(a, b, preferred_element_type=jnp.float32)


def gather_kernel(
    x_hbm, buf, xr, xv, lane_w, row_w, part, starts, halves, tot, trecv,
    load_sem, send_sem, first_sem, second_sem, tot_send, tot_recv, row_sem, ready_sem,
):
    me = lax.axis_index("dev")
    grp = lax.axis_index("grp")
    y, x, z, c = me // 16, (me // 4) % 4, (me // 2) % 2, me % 2

    def remote(src, dst, ssem, rsem, dev):
        return pltpu.make_async_remote_copy(
            src_ref=src, dst_ref=dst, send_sem=ssem, recv_sem=rsem,
            device_id={"dev": dev}, device_id_type=MESH,
        )

    barrier = pltpu.get_barrier_semaphore()

    def device(o, sign=1):
        return (
            ((y + sign * o[0] + 4) % 4) * 16
            + ((x + sign * o[1] + 4) % 4) * 4
            + ((z + o[2]) % 2) * 2
            + (c + o[3]) % 2
        )

    for o in NEAR:
        pl.semaphore_signal(barrier, inc=1, device_id={"dev": device(o)}, device_id_type=MESH)

    def greet(g, _):
        pl.semaphore_signal(barrier, inc=1, device_id={"grp": g}, device_id_type=MESH)
        return 0

    lax.fori_loop(grp + 1, GROUPS, greet, 0)
    loads = []
    for i in range(4):
        ts = pl.ds(((y + i) % 4) * 16, 16)
        loads.append(pltpu.make_async_copy(x_hbm.at[ts], xr.at[ts], load_sem.at[i]))
        loads[-1].start()

    pl.semaphore_wait(barrier, len(NEAR) + grp)
    for i in range(1, 4):
        pl.semaphore_signal(
            row_sem, inc=1, device_id={"dev": device((i, 0, 0, 0))}, device_id_type=MESH
        )

    def send_first(order):
        half = pl.ds(0, HALF)
        for o in order:
            t = device(o)
            remote(x_hbm.at[t, half], buf.at[me, half], send_sem, first_sem.at[me], t).start()

    send_first(ORDER[1:NOW])

    def ready(g, _):
        pl.semaphore_signal(ready_sem, inc=1, device_id={"grp": g}, device_id_type=MESH)
        return 0

    lax.fori_loop(0, grp, ready, 0)

    r = lax.broadcasted_iota(jnp.int32, (2 * LANES, 2 * LANES), 0) % LANES
    q = lax.broadcasted_iota(jnp.int32, (2 * LANES, 2 * LANES), 1)
    lane_w[...] = ((r < q) | (q >= LANES)).astype(jnp.float32).astype(jnp.bfloat16)
    r = lax.broadcasted_iota(jnp.int32, (ROWS, 2 * ROWS), 0)
    q = lax.broadcasted_iota(jnp.int32, (ROWS, 2 * ROWS), 1) % ROWS
    row_w[...] = (q < r).astype(jnp.float32).astype(jnp.bfloat16)

    def lane_scan(v):
        hi, mid, lo = split3(v)
        return dot(jnp.concatenate([hi, mid], axis=1), lane_w[...]) + dot(lo, lane_w[0:LANES])

    def scan(ts):
        both = lane_scan(jnp.concatenate([xr[t] for t in ts], axis=0))
        out = []
        for k in range(len(ts)):
            rows = slice(k * ROWS, (k + 1) * ROWS)
            a, b, d = split3(both[rows, LANES:])
            before = dot(row_w[...], jnp.concatenate([a, b], axis=0)) + dot(row_w[:, 0:ROWS], d)
            out.append(both[rows, :LANES] + before)
        for t, v in zip(ts, out):
            xv[t] = v

    pl.semaphore_wait(row_sem, 3)
    send_first(ORDER[NOW:SOON])
    for load in loads:
        load.wait()

    def range_sum(t, _):
        part[t] = jnp.sum(xr[t].reshape(ROWS // 8, 8, LANES), axis=0)
        return 0

    lax.fori_loop(0, N, range_sum, 0)
    sums = jnp.sum(jnp.sum(part[...], axis=1), axis=1, keepdims=True)
    sums = jnp.broadcast_to(sums, (N, LANES))
    tot[...] = jnp.broadcast_to(jnp.sum(sums, axis=0, keepdims=True), (8, LANES))
    low = row_w[0:N, 0:N]
    a, b, d = split3(sums)
    starts[...] = dot(low, a) + dot(low, b) + dot(low, d)

    @pl.when(grp < GROUPS - 1)
    def _():
        pl.semaphore_wait(ready_sem, GROUPS - 1 - grp)

    def send_total(g, _):
        pltpu.make_async_remote_copy(
            src_ref=tot, dst_ref=trecv.at[grp], send_sem=tot_send.at[g], recv_sem=tot_recv.at[grp],
            device_id={"grp": g}, device_id_type=MESH,
        ).start()
        return 0

    lax.fori_loop(grp + 1, GROUPS, send_total, 0)
    send_first(ORDER[SOON:])

    table = [[o[k] for o in ORDER] for k in range(4)]

    def devices(i, sign=1):
        return [device([pick(i, v[m::STEP]) for v in table], sign) for m in range(STEP)]

    def scan_step(i, _):
        scan(devices(i))
        return 0

    lax.fori_loop(0, N // STEP, scan_step, 0)

    def add_total(g, base):
        pltpu.make_async_copy(tot, tot, tot_recv.at[g]).wait()
        return base + trecv[g]

    base = lax.fori_loop(0, grp, add_total, jnp.zeros((8, LANES), jnp.float32))

    def put_start(t, _):
        xv[t] += starts[pl.ds(t, 1)] + base[0:1]
        return 0

    lax.fori_loop(0, N, put_start, 0)
    for o in ORDER[1:]:
        t, half = device(o), pl.ds(HALF, HALF)
        remote(xv.at[t, half], buf.at[me, half], send_sem, second_sem.at[me], t).start()
    buf[me] = xv[me]

    low_half = row_w[0:HALF, 0:HALF]

    def scan_first(srcs):
        for src in srcs:
            half = buf.at[src, pl.ds(0, HALF)]
            pltpu.make_async_copy(half, half, first_sem.at[src]).wait()
        both = lane_scan(jnp.concatenate([buf[src, 0:HALF] for src in srcs], axis=0))
        out = []
        for k in range(len(srcs)):
            rows = slice(k * HALF, (k + 1) * HALF)
            sums = both[rows, LANES:]
            a, b, d = split3(sums)
            before = dot(low_half, a) + dot(low_half, b) + dot(low_half, d)
            out.append((both[rows, :LANES] + before, (before + sums)[HALF - 1 :]))
        for src, (v, total) in zip(srcs, out):
            buf[src, 0:HALF] = v
            halves[pl.ds(src, 1)] = total

    scan_first([device(o, -1) for o in ORDER[1:STEP]])

    def first_step(i, _):
        scan_first(devices(i, -1))
        return 0

    lax.fori_loop(1, N // STEP, first_step, 0)

    for i in range(0, N, LAST):
        srcs = [device(o, -1) for o in ORDER[max(i, 1) : i + LAST]]
        for src in srcs:
            half = buf.at[src, pl.ds(HALF, HALF)]
            pltpu.make_async_copy(half, half, second_sem.at[src]).wait()
        heads = [jnp.broadcast_to(buf[src, HALF : HALF + 1, 0:1], (1, LANES)) for src in srcs]
        out = [buf[src, 0:HALF] + (h - halves[pl.ds(src, 1)]) for src, h in zip(srcs, heads)]
        for src, v in zip(srcs, out):
            buf[src, 0:HALF] = v

    def total_sent(g, _):
        pltpu.make_async_copy(tot, tot, tot_send.at[g]).wait()
        return 0

    lax.fori_loop(grp + 1, GROUPS, total_sent, 0)
    sent = buf.at[pl.ds(0, N - 1)]
    pltpu.make_async_copy(sent, sent, send_sem).wait()


def place_kernel(buf, out, sem):
    for t in range(N):
        pltpu.make_async_copy(buf.at[t], out.at[t // 8, :, t % 8], sem).start()
    pltpu.make_async_copy(out, out, sem).wait()


def local(amounts):
    slabs = amounts.reshape(N, ROWS, LANES)
    f32, bf16, dma = jnp.float32, jnp.bfloat16, pltpu.SemaphoreType.DMA
    buf = pl.pallas_call(
        gather_kernel,
        out_shape=pltpu.VMEM((N, ROWS, LANES), f32),
        in_specs=[pl.BlockSpec(memory_space=pltpu.HBM)],
        out_specs=pl.BlockSpec(memory_space=pltpu.VMEM),
        scratch_shapes=[
            pltpu.VMEM((N, ROWS, LANES), f32),
            pltpu.VMEM((N, ROWS, LANES), f32),
            pltpu.VMEM((2 * LANES, 2 * LANES), bf16),
            pltpu.VMEM((ROWS, 2 * ROWS), bf16),
            pltpu.VMEM((N, 8, LANES), f32),
            pltpu.VMEM((N, LANES), f32),
            pltpu.VMEM((N, LANES), f32),
            pltpu.VMEM((8, LANES), f32),
            pltpu.VMEM((GROUPS, 8, LANES), f32),
            dma((4,)), dma, dma((N,)), dma((N,)), dma((GROUPS,)), dma((GROUPS,)),
            pltpu.SemaphoreType.REGULAR, pltpu.SemaphoreType.REGULAR,
        ],
        compiler_params=pltpu.CompilerParams(
            collective_id=0, has_side_effects=True, vmem_limit_bytes=56 * 2**20
        ),
    )(slabs)
    out = pl.pallas_call(
        place_kernel,
        out_shape=jax.ShapeDtypeStruct((8, ROWS, 8, LANES), f32),
        in_specs=[pl.BlockSpec(memory_space=pltpu.VMEM)],
        out_specs=pl.BlockSpec(memory_space=pltpu.HBM),
        scratch_shapes=[dma],
        compiler_params=pltpu.CompilerParams(vmem_limit_bytes=8 * 2**20),
    )(pltpu.with_memory_space_constraint(buf, pltpu.VMEM))
    return out.transpose(0, 2, 1, 3).reshape(N, ROWS * LANES)


def solution(mesh):
    return jax.shard_map(
        local,
        mesh=mesh,
        in_specs=(P("dev", "grp"),),
        out_specs=P(None, ("grp", "dev")),
        check_vma=False,
    )
```

```python
import jax
import jax.numpy as jnp
from jax import lax
from jax.experimental import pallas as pl
from jax.experimental.pallas import tpu as pltpu
from jax.sharding import PartitionSpec as P

MESH = pl.DeviceIdType.MESH
LANES = 128
ROWS = 128
N = 64
GROUPS = 4
HALF = ROWS // 2
PLANE = [(0, w // 4, w // 2 % 2, w % 2) for w in range(1, 16)]
LINE = [(i, 0, 0, k) for k in range(2) for i in range(1, 4)]
NEAR = PLANE[::-1] + LINE
STEP = 4
LAST = 8


def order():
    first = [(0, 0, 0, 0)]
    for k in range(2):
        first += [(0, 0, 1, k), (0, 1, 0, k), (1, 0, 0, k), (0, 3, 0, k), (3, 0, 0, k)]
    first.append((0, 0, 0, 1))
    near = [(2, 0, 0, 0), (0, 2, 0, 0), (2, 0, 0, 1), (0, 1, 1, 1), (0, 3, 1, 0)]
    near += [(0, 2, 1, 0), (0, 2, 0, 1), (0, 1, 1, 0), (0, 3, 1, 1), (0, 2, 1, 1)]
    far = [[(1 + k, w // 4, w // 2 % 2, w % 2) for w in range(2, 16)] for k in range(3)]
    rest = []
    for i in range(14):
        rest += [far[k][(5 * i + 4 * k + 3) % 14] for k in range(3)]
        if i * 10 // 14 != (i + 1) * 10 // 14:
            rest.append(near.pop((3 * len(rest) // 5) % len(near)))
    return first + rest


ORDER = order()
NOW = 12
SOON = 36


def pick(i, values):
    r = values[0]
    for k, v in enumerate(values[1:], 1):
        r = jnp.where(i == k, v, r)
    return r


def split3(v):
    hi = v.astype(jnp.bfloat16)
    rest = v - hi.astype(jnp.float32)
    mid = rest.astype(jnp.bfloat16)
    lo = (rest - mid.astype(jnp.float32)).astype(jnp.bfloat16)
    return hi, mid, lo


def dot(a, b):
    return jnp.dot(a, b, preferred_element_type=jnp.float32)


def gather_kernel(
    x_hbm, buf, xr, xv, lane_w, row_w, part, starts, halves, tot, trecv,
    load_sem, send_sem, first_sem, second_sem, tot_send, tot_recv, row_sem, ready_sem,
):
    me = lax.axis_index("dev")
    grp = lax.axis_index("grp")
    y, x, z, c = me // 16, (me // 4) % 4, (me // 2) % 2, me % 2

    def remote(src, dst, ssem, rsem, dev):
        return pltpu.make_async_remote_copy(
            src_ref=src, dst_ref=dst, send_sem=ssem, recv_sem=rsem,
            device_id={"dev": dev}, device_id_type=MESH,
        )

    barrier = pltpu.get_barrier_semaphore()

    def device(o, sign=1):
        return (
            ((y + sign * o[0] + 4) % 4) * 16
            + ((x + sign * o[1] + 4) % 4) * 4
            + ((z + o[2]) % 2) * 2
            + (c + o[3]) % 2
        )

    for o in NEAR:
        pl.semaphore_signal(barrier, inc=1, device_id={"dev": device(o)}, device_id_type=MESH)

    def greet(g, _):
        pl.semaphore_signal(barrier, inc=1, device_id={"grp": g}, device_id_type=MESH)
        return 0

    lax.fori_loop(grp + 1, GROUPS, greet, 0)
    loads = []
    for i in range(4):
        ts = pl.ds(((y + i) % 4) * 16, 16)
        loads.append(pltpu.make_async_copy(x_hbm.at[ts], xr.at[ts], load_sem.at[i]))
        loads[-1].start()

    pl.semaphore_wait(barrier, len(NEAR) + grp)
    for i in range(1, 4):
        pl.semaphore_signal(
            row_sem, inc=1, device_id={"dev": device((i, 0, 0, 0))}, device_id_type=MESH
        )

    def send_first(order):
        half = pl.ds(0, HALF)
        for o in order:
            t = device(o)
            remote(x_hbm.at[t, half], buf.at[me, half], send_sem, first_sem.at[me], t).start()

    send_first(ORDER[1:NOW])

    def ready(g, _):
        pl.semaphore_signal(ready_sem, inc=1, device_id={"grp": g}, device_id_type=MESH)
        return 0

    lax.fori_loop(0, grp, ready, 0)

    r = lax.broadcasted_iota(jnp.int32, (2 * LANES, 2 * LANES), 0) % LANES
    q = lax.broadcasted_iota(jnp.int32, (2 * LANES, 2 * LANES), 1)
    lane_w[...] = ((r < q) | (q >= LANES)).astype(jnp.float32).astype(jnp.bfloat16)
    r = lax.broadcasted_iota(jnp.int32, (ROWS, 2 * ROWS), 0)
    q = lax.broadcasted_iota(jnp.int32, (ROWS, 2 * ROWS), 1) % ROWS
    row_w[...] = (q < r).astype(jnp.float32).astype(jnp.bfloat16)

    def lane_scan(v):
        hi, mid, lo = split3(v)
        return dot(jnp.concatenate([hi, mid], axis=1), lane_w[...]) + dot(lo, lane_w[0:LANES])

    def scan(ts):
        both = lane_scan(jnp.concatenate([xr[t] for t in ts], axis=0))
        out = []
        for k in range(len(ts)):
            rows = slice(k * ROWS, (k + 1) * ROWS)
            a, b, d = split3(both[rows, LANES:])
            before = dot(row_w[...], jnp.concatenate([a, b], axis=0)) + dot(row_w[:, 0:ROWS], d)
            out.append(both[rows, :LANES] + before)
        for t, v in zip(ts, out):
            xv[t] = v

    for load in loads:
        load.wait()

    def range_sum(t, _):
        part[t] = jnp.sum(xr[t].reshape(ROWS // 8, 8, LANES), axis=0)
        return 0

    lax.fori_loop(0, N, range_sum, 0)
    sums = jnp.sum(jnp.sum(part[...], axis=1), axis=1, keepdims=True)
    sums = jnp.broadcast_to(sums, (N, LANES))
    tot[...] = jnp.broadcast_to(jnp.sum(sums, axis=0, keepdims=True), (8, LANES))
    low = row_w[0:N, 0:N]
    a, b, d = split3(sums)
    starts[...] = dot(low, a) + dot(low, b) + dot(low, d)

    pl.semaphore_wait(row_sem, 3)
    send_first(ORDER[NOW:SOON])

    @pl.when(grp < GROUPS - 1)
    def _():
        pl.semaphore_wait(ready_sem, GROUPS - 1 - grp)

    def send_total(g, _):
        pltpu.make_async_remote_copy(
            src_ref=tot, dst_ref=trecv.at[grp], send_sem=tot_send.at[g], recv_sem=tot_recv.at[grp],
            device_id={"grp": g}, device_id_type=MESH,
        ).start()
        return 0

    lax.fori_loop(grp + 1, GROUPS, send_total, 0)
    send_first(ORDER[SOON:])

    table = [[o[k] for o in ORDER] for k in range(4)]

    def devices(i, sign=1):
        return [device([pick(i, v[m::STEP]) for v in table], sign) for m in range(STEP)]

    def scan_step(i, _):
        scan(devices(i))
        return 0

    lax.fori_loop(0, N // STEP, scan_step, 0)

    def add_total(g, base):
        pltpu.make_async_copy(tot, tot, tot_recv.at[g]).wait()
        return base + trecv[g]

    base = lax.fori_loop(0, grp, add_total, jnp.zeros((8, LANES), jnp.float32))

    def put_start(t, _):
        xv[t] += starts[pl.ds(t, 1)] + base[0:1]
        return 0

    lax.fori_loop(0, N, put_start, 0)
    for o in ORDER[1:]:
        t, half = device(o), pl.ds(HALF, HALF)
        remote(xv.at[t, half], buf.at[me, half], send_sem, second_sem.at[me], t).start()
    buf[me] = xv[me]

    low_half = row_w[0:HALF, 0:HALF]

    def scan_first(srcs):
        for src in srcs:
            half = buf.at[src, pl.ds(0, HALF)]
            pltpu.make_async_copy(half, half, first_sem.at[src]).wait()
        both = lane_scan(jnp.concatenate([buf[src, 0:HALF] for src in srcs], axis=0))
        out = []
        for k in range(len(srcs)):
            rows = slice(k * HALF, (k + 1) * HALF)
            sums = both[rows, LANES:]
            a, b, d = split3(sums)
            before = dot(low_half, a) + dot(low_half, b) + dot(low_half, d)
            out.append((both[rows, :LANES] + before, (before + sums)[HALF - 1 :]))
        for src, (v, total) in zip(srcs, out):
            buf[src, 0:HALF] = v
            halves[pl.ds(src, 1)] = total

    scan_first([device(o, -1) for o in ORDER[1:STEP]])

    def first_step(i, _):
        scan_first(devices(i, -1))
        return 0

    lax.fori_loop(1, N // STEP, first_step, 0)

    for i in range(0, N, LAST):
        srcs = [device(o, -1) for o in ORDER[max(i, 1) : i + LAST]]
        for src in srcs:
            half = buf.at[src, pl.ds(HALF, HALF)]
            pltpu.make_async_copy(half, half, second_sem.at[src]).wait()
        heads = [jnp.broadcast_to(buf[src, HALF : HALF + 1, 0:1], (1, LANES)) for src in srcs]
        out = [buf[src, 0:HALF] + (h - halves[pl.ds(src, 1)]) for src, h in zip(srcs, heads)]
        for src, v in zip(srcs, out):
            buf[src, 0:HALF] = v

    def total_sent(g, _):
        pltpu.make_async_copy(tot, tot, tot_send.at[g]).wait()
        return 0

    lax.fori_loop(grp + 1, GROUPS, total_sent, 0)
    sent = buf.at[pl.ds(0, N - 1)]
    pltpu.make_async_copy(sent, sent, send_sem).wait()


def place_kernel(buf, out, sem):
    for t in range(N):
        pltpu.make_async_copy(buf.at[t], out.at[t // 8, :, t % 8], sem).start()
    pltpu.make_async_copy(out, out, sem).wait()


def local(amounts):
    slabs = amounts.reshape(N, ROWS, LANES)
    f32, bf16, dma = jnp.float32, jnp.bfloat16, pltpu.SemaphoreType.DMA
    buf = pl.pallas_call(
        gather_kernel,
        out_shape=pltpu.VMEM((N, ROWS, LANES), f32),
        in_specs=[pl.BlockSpec(memory_space=pltpu.HBM)],
        out_specs=pl.BlockSpec(memory_space=pltpu.VMEM),
        scratch_shapes=[
            pltpu.VMEM((N, ROWS, LANES), f32),
            pltpu.VMEM((N, ROWS, LANES), f32),
            pltpu.VMEM((2 * LANES, 2 * LANES), bf16),
            pltpu.VMEM((ROWS, 2 * ROWS), bf16),
            pltpu.VMEM((N, 8, LANES), f32),
            pltpu.VMEM((N, LANES), f32),
            pltpu.VMEM((N, LANES), f32),
            pltpu.VMEM((8, LANES), f32),
            pltpu.VMEM((GROUPS, 8, LANES), f32),
            dma((4,)), dma, dma((N,)), dma((N,)), dma((GROUPS,)), dma((GROUPS,)),
            pltpu.SemaphoreType.REGULAR, pltpu.SemaphoreType.REGULAR,
        ],
        compiler_params=pltpu.CompilerParams(
            collective_id=0, has_side_effects=True, vmem_limit_bytes=56 * 2**20
        ),
    )(slabs)
    out = pl.pallas_call(
        place_kernel,
        out_shape=jax.ShapeDtypeStruct((8, ROWS, 8, LANES), f32),
        in_specs=[pl.BlockSpec(memory_space=pltpu.VMEM)],
        out_specs=pl.BlockSpec(memory_space=pltpu.HBM),
        scratch_shapes=[dma],
        compiler_params=pltpu.CompilerParams(vmem_limit_bytes=8 * 2**20),
    )(pltpu.with_memory_space_constraint(buf, pltpu.VMEM))
    return out.transpose(0, 2, 1, 3).reshape(N, ROWS * LANES)


def solution(mesh):
    return jax.shard_map(
        local,
        mesh=mesh,
        in_specs=(P("dev", "grp"),),
        out_specs=P(None, ("grp", "dev")),
        check_vma=False,
    )
```
